512 devices in a mesh: seq: 32 (over z, core), head: 4 (over x), pool: 4 (over y).
Axes of the slice: x: 4, y: 4, z: 16, core: 2. Of those that a mesh axis runs over, the one named last changes fastest.
Arguments:
- tokens: bfloat16 [512, 4096], P(('seq', 'head'), 'pool'), may hold values from -6 to 6
- routes: int32 [512, 8], P(('seq', 'head')), may hold values from 0 to 31, all different within a row; in each aligned block of 4 rows (0 to 3, 4 to 7, ...) at most 2 rows name the same one
- gate_fixed: int32 [512, 8], P(('seq', 'head')), may hold values from 1 to 65535
- gate_weight: bfloat16 [32, 4096, 3072], P('seq', 'pool', 'head'), may hold values from -0.09375 to 0.09375
- up_weight: bfloat16 [32, 4096, 3072], P('seq', 'pool', 'head'), may hold values from -0.09375 to 0.09375
- down_weight: bfloat16 [32, 3072, 4096], P('seq', 'head', 'pool'), may hold values from -0.109375 to 0.109375
- gate_scale: bfloat16 [32, 32, 24], P('seq', 'pool', 'head'), may hold values from 0.5 to 2
- up_scale: bfloat16 [32, 32, 24], P('seq', 'pool', 'head'), may hold values from 0.5 to 2
- down_scale: bfloat16 [32, 24, 32], P('seq', 'head', 'pool'), may hold values from 0.5 to 2
Outputs:
- combined: bfloat16 [512, 4096], P(('seq', 'head'), 'pool')
The draws below stay inside these ranges and needn't reach their ends.
Inputs may be any that keep to these rules, and one draw needn't show every extreme that they name: `routes`: each row names 8 different experts. Within the rows of one device (aligned blocks of 4 rows) no expert is named by more than 2 rows, and in some blocks one expert is named by exactly 2 rows.
All inputs are finite; a program needn't handle non-finite values.
Results may differ from the reference program's by a relative error of at most 0.02.
Values may be sent and summed in bfloat16 or wider, within the bound.
A program may use at most 64 MiB of HBM per device.

```python
import math
import jax
import jax.numpy as jnp
import numpy as np
from jax import lax

D = 4096
FF = 3072
TOP = 8
QB = 128
ROWS_DEV = 4
CAP = 2
EXPERTS = 32
BLOCKS = 128
ROWS = 512
N_HEAD = 4
N_POOL = 4


def place_ends(entries, rng, low, top_value):
    longest = entries.shape.index(max(entries.shape))
    spots = []
    for shift in (0, 1):
        where = [jax.random.randint(jax.random.fold_in(rng, axis), (), 0, length) for axis, length in enumerate(entries.shape)]
        where[longest] = (where[longest] + shift) % entries.shape[longest]
        spots.append(tuple(where))
    return entries.at[spots[0]].set(low).at[spots[1]].set(top_value)


def block_levels(stream_key, extent, cuts, least, top_value):
    def one(dim, blocks):
        steps = jax.random.uniform(jax.random.fold_in(jax.random.fold_in(stream_key, 6), dim), (blocks,), jnp.float32, least / len(cuts), top_value / len(cuts))
        return jnp.repeat(jnp.exp(steps), extent[dim] // blocks).reshape((-1,) + (1,) * (len(extent) - dim - 1))

    level = one(*cuts[0])
    for cut in cuts[1:]:
        level = level * one(*cut)
    return level


def assign_block(key, own, number, rows, number_of, top, most, lean):
    ranking = jax.random.permutation(key, number_of)
    packed, usual = load_shares(number_of, rows * top, most, lean, True), load_shares(number_of, rows * top, most, lean, False)
    places = jnp.arange(number_of)

    def named(tallies, turn):
        used = int((tallies > 0).sum())
        fixed = max(1, used // 4)
        passed = fixed + (places - fixed + turn * (used - fixed)) % max(1, number_of - fixed)
        return jnp.zeros((number_of,), jnp.int32).at[ranking[jnp.where(places < fixed, places, passed)]].set(jnp.asarray(tallies, jnp.int32))

    tallies = jnp.where(number % 4 == 0, named(packed, number // 4), named(usual, number - number // 4 - 1))
    mixed = jax.random.permutation(jax.random.fold_in(own, 3), number_of)
    source_of, sink = mixed[0:number_of // 2 * 2:2], mixed[1:number_of // 2 * 2:2]
    margin = jnp.minimum(tallies[source_of] - 1, most - tallies[sink]) // 2
    margin = jnp.where((source_of == ranking[0]) | (sink == ranking[0]) | (tallies[sink] == 0), 0, jnp.maximum(margin, 0))
    passed = jax.random.randint(jax.random.fold_in(own, 4), (number_of // 2,), 0, 1 << 20) % (margin + 1)
    tallies = tallies.at[source_of].add(-passed).at[sink].add(passed)
    members = jnp.searchsorted(jnp.cumsum(tallies), jnp.arange(rows * top), side="right").astype(jnp.int32)
    grid = members.reshape(top, rows).T
    grid = grid[jax.random.permutation(jax.random.fold_in(own, 1), rows)]
    turn = jax.random.randint(jax.random.fold_in(own, 2), (rows, 1), 0, top)
    return jnp.take_along_axis(grid, (jnp.arange(top)[None, :] + turn) % top, axis=1)


def load_shares(amount, total, reach, skew, full):
    portions = [(1 << 20) // math.isqrt(rank ** skew) + 1 for rank in range(1, amount + 1)]
    largest = reach if full else min(reach, max(-(-total // amount), total * portions[0] // sum(portions)))
    least = 1 if total - largest >= amount - 1 else 0
    counts, rest = [largest] + [least] * (amount - 1), total - largest - least * (amount - 1)
    while rest > 0:
        candidates = [i for i in range(1, amount) if counts[i] < largest] or [i for i in range(1, amount) if counts[i] < reach]
        whole, remaining = sum([portions[i] for i in candidates]), rest
        for i in candidates:
            more = min(reach - counts[i], max(1, remaining * portions[i] // whole), rest)
            counts[i] = counts[i] + more
            rest = rest - more
    return np.array(counts)


def centred(stream_key, shape, deviation, limit, cuts=(), kind=jnp.bfloat16):
    entries = deviation * jax.random.normal(stream_key, shape, jnp.float32)
    if cuts:
        entries = entries * block_levels(stream_key, shape, cuts, -0.22, 0.18)
    return jnp.clip(entries, -limit, limit).astype(kind)


def setup_inputs(seed: int = 0) -> dict:
    key_of = jax.random.split(jax.random.key(seed), 10)
    tokens = centred(key_of[0], (ROWS, D), 1.0, 6.0, ((0, 128), (1, 4)))
    routes_keys = jax.random.split(jax.random.fold_in(key_of[1], 1), ROWS // ROWS_DEV)
    routes_turns = jax.random.permutation(jax.random.fold_in(key_of[1], 3), ROWS // ROWS_DEV)
    routes = jax.vmap(lambda own, number: assign_block(jax.random.fold_in(key_of[1], 2), own, number, ROWS_DEV, EXPERTS, TOP, CAP, 2))(routes_keys, routes_turns).reshape((ROWS, TOP))
    gate_fixed = place_ends(jax.random.randint(key_of[2], (ROWS, TOP), 1, 65536), jax.random.fold_in(key_of[2], 1), 1, 65535).astype(jnp.int32)
    gate_weight = centred(key_of[3], (EXPERTS, D, FF), D ** -0.5, 0.09375, ((0, 32), (1, 4), (2, 4)))
    up_weight = centred(key_of[4], (EXPERTS, D, FF), D ** -0.5, 0.09375, ((0, 32), (1, 4), (2, 4)))
    down_weight = centred(key_of[5], (EXPERTS, FF, D), FF ** -0.5, 0.109375, ((0, 32), (1, 4), (2, 4)))
    gate_scale = jnp.clip(jnp.exp(math.log(2.0) - 1.3862944 * jax.random.uniform(key_of[6], (EXPERTS, D // QB, FF // QB), jnp.float32) ** block_levels(key_of[6], (EXPERTS, D // QB, FF // QB), ((0, 32), (1, 4), (2, 4)), -0.2, 0.2)), 0.5, 2.0).astype(jnp.bfloat16)
    up_scale = jnp.clip(jnp.exp(math.log(2.0) - 1.3862944 * jax.random.uniform(key_of[7], (EXPERTS, D // QB, FF // QB), jnp.float32) ** block_levels(key_of[7], (EXPERTS, D // QB, FF // QB), ((0, 32), (1, 4), (2, 4)), -0.2, 0.2)), 0.5, 2.0).astype(jnp.bfloat16)
    down_scale = jnp.clip(jnp.exp(math.log(2.0) - 1.3862944 * jax.random.uniform(key_of[8], (EXPERTS, FF // QB, D // QB), jnp.float32) ** block_levels(key_of[8], (EXPERTS, FF // QB, D // QB), ((0, 32), (1, 4), (2, 4)), -0.2, 0.2)), 0.5, 2.0).astype(jnp.bfloat16)
    return dict(tokens=tokens, routes=routes, gate_fixed=gate_fixed, gate_weight=gate_weight, up_weight=up_weight, down_weight=down_weight, gate_scale=gate_scale, up_scale=up_scale, down_scale=down_scale)


largest_choice = lax.Precision.HIGHEST


def expand_scale(route_weight, scale):
    grown = jnp.repeat(jnp.repeat(scale.astype(jnp.float32), QB, axis=0), QB, axis=1)
    return (route_weight.astype(jnp.float32) * grown).astype(jnp.bfloat16)


def slot_positions(block_routes):
    flattened = block_routes.reshape(-1)
    expert_ids = jnp.arange(EXPERTS, dtype=jnp.int32)
    onehot = (flattened[:, None] == expert_ids[None, :]).astype(jnp.int32)
    before = jnp.cumsum(onehot, axis=0) - onehot
    slot_index = jnp.sum(before * onehot, axis=1)
    return (flattened * CAP + slot_index).reshape(block_routes.shape)


def expert_apply(operands):
    slot_rows, gate_weight, up_weight, down_weight, gate_scale, up_scale, down_scale = operands
    gate_dense = expand_scale(gate_weight, gate_scale)
    up_dense = expand_scale(up_weight, up_scale)
    down_dense = expand_scale(down_weight, down_scale)
    slot_count = slot_rows.shape[0]
    pooled = slot_rows.astype(jnp.float32).reshape(slot_count, N_POOL, D // N_POOL)

    def pool_sum(dense):
        grouped = dense.astype(jnp.float32).reshape(N_POOL, D // N_POOL, FF)
        partial_results = jnp.einsum("mpd,pdf->pmf", pooled, grouped, precision=largest_choice)
        rounded = lax.optimization_barrier(partial_results.astype(jnp.bfloat16))
        return jnp.sum(rounded.astype(jnp.float32), axis=0)

    gate_sum = pool_sum(gate_dense)
    up_sum = pool_sum(up_dense)
    hidden = (jax.nn.silu(gate_sum) * up_sum).astype(jnp.bfloat16)
    hidden_parts = hidden.astype(jnp.float32).reshape(slot_count, N_HEAD, FF // N_HEAD)
    down_by_expert = down_dense.astype(jnp.float32).reshape(N_HEAD, FF // N_HEAD, D)
    partial_results = jnp.einsum("vct,ctq->cvq", hidden_parts, down_by_expert, precision=largest_choice)
    rounded = lax.optimization_barrier(partial_results.astype(jnp.bfloat16))
    return jnp.sum(rounded.astype(jnp.float32), axis=0).astype(jnp.bfloat16)


def reference(tokens, routes, gate_fixed, gate_weight, up_weight, down_weight, gate_scale, up_scale, down_scale):
    blocked = routes.reshape(BLOCKS, ROWS_DEV, TOP)
    positions = jax.vmap(slot_positions)(blocked)
    targets = jnp.arange(EXPERTS * CAP, dtype=jnp.int32)
    matches = jnp.any(positions[:, :, :, None] == targets[None, None, None, :], axis=2).astype(jnp.int32)
    row_local = jnp.arange(ROWS_DEV, dtype=jnp.int32)
    found = jnp.sum(matches, axis=1)
    local_row = jnp.sum(matches * row_local[None, :, None], axis=1)
    block_start = (jnp.arange(BLOCKS, dtype=jnp.int32) * ROWS_DEV)[:, None]
    source = jnp.where(found > 0, block_start + local_row, ROWS).astype(jnp.int32)
    padded = jnp.concatenate([tokens, jnp.zeros((1, D), tokens.dtype)], axis=0)
    gathered = padded[source]
    per_expert = gathered.reshape(BLOCKS, EXPERTS, CAP, D).transpose(1, 0, 2, 3).reshape(EXPERTS, BLOCKS * CAP, D)
    outputs = lax.map(expert_apply, (per_expert, gate_weight, up_weight, down_weight, gate_scale, up_scale, down_scale))
    outputs = outputs.reshape(EXPERTS, BLOCKS, CAP, D)
    slot_index = (positions - blocked * CAP).astype(jnp.int32)
    block_ids = jnp.arange(BLOCKS, dtype=jnp.int32)[:, None, None]
    picked = outputs[blocked, block_ids, slot_index]
    fixed = gate_fixed.astype(jnp.float32).reshape(BLOCKS, ROWS_DEV, TOP)
    weights = fixed / jnp.sum(fixed, axis=2, keepdims=True)
    combined = jnp.sum(weights[..., None] * picked.astype(jnp.float32), axis=2)
    return combined.reshape(ROWS, D).astype(jnp.bfloat16)
```

```python
import functools

import jax
import jax.numpy as jnp
from jax import lax
from jax.experimental import pallas as pl
from jax.experimental.pallas import tpu as pltpu
from jax.sharding import PartitionSpec as P

QB = 128
CAP = 2
NX = 4
CHUNKS = 4
F32 = jnp.float32
BF16 = jnp.bfloat16


def offset(i):
    k = (i + 1) // 2
    return k if i % 2 == 0 else -k


def opposite(i, nz):
    if i == 0:
        return 0
    other = i + 1 if i % 2 else i - 1
    return other if other < nz else i


class Copies:
    def __init__(self):
        self.sent = []

    def make(self, src, dst, send, recv, device):
        return pltpu.make_async_remote_copy(
            src_ref=src,
            dst_ref=dst,
            send_sem=send,
            recv_sem=recv,
            device_id=device,
            device_id_type=pl.DeviceIdType.MESH,
        )

    def start(self, *args):
        copy = self.make(*args)
        copy.start()
        self.sent.append(copy)


def kernel(
    nz,
    tokens_hbm,
    routes_hbm,
    fixed_hbm,
    gate_hbm,
    up_hbm,
    down_hbm,
    gs_hbm,
    us_hbm,
    ds_hbm,
    out_ref,
    tokens,
    routes,
    fixed,
    w1,
    w2,
    gs,
    us,
    ds_,
    grown1,
    grown2,
    slots,
    gathered,
    wide,
    x_ref,
    partial,
    relay_y,
    sums_y,
    arrive_y,
    hidden,
    outs,
    relay_x,
    sums_x,
    arrive_x,
    back_wide,
    back,
    results,
    load_sem,
    zs,
    zr,
    gx_s,
    gx_r,
    ry_s,
    ry_r,
    gy_s,
    gy_r,
    rx_s,
    rx_r,
    bs,
    br,
):
    s = lax.axis_index("seq")
    h = lax.axis_index("head")
    p = lax.axis_index("pool")
    z = s // 2
    core = s % 2
    nc = CHUNKS
    ni = nz // nc
    ne = 2 * nz
    m = NX * ni * 2 * CAP
    share = m // NX
    f1 = w1.shape[1] // 2
    dw = w2.shape[1]
    jw = dw // 128

    def near(base, step):
        return (base + step + NX) % NX

    xr, xl, xo = near(h, 1), near(h, -1), near(h, 2)
    yr, yl, yo = near(p, 1), near(p, -1), near(p, 2)
    dev_xr, dev_xl = (s, xr, p), (s, xl, p)
    dev_yr, dev_yl = (s, h, yr), (s, h, yl)

    def chip(i, to_core):
        return (((z + offset(i) + nz) % nz) * 2 + to_core, h, p)

    peers = [(i, c) for i in range(nz) for c in (0, 1)]

    barrier = pltpu.get_barrier_semaphore()
    for i in range(nz - 1, 0, -1):
        for c in (0, 1):
            pl.semaphore_signal(barrier, inc=1, device_id=chip(i, c), device_id_type=pl.DeviceIdType.MESH)
    for dev in (chip(0, 1 - core), dev_xr, dev_xl, dev_yr, dev_yl):
        pl.semaphore_signal(barrier, inc=1, device_id=dev, device_id_type=pl.DeviceIdType.MESH)

    loads = [
        (tokens_hbm, tokens),
        (routes_hbm, routes),
        (fixed_hbm, fixed),
        (gs_hbm, gs),
        (us_hbm, us),
        (ds_hbm, ds_),
        (gate_hbm.at[0], w1.at[:, pl.ds(0, f1)]),
        (up_hbm.at[0], w1.at[:, pl.ds(f1, f1)]),
        (down_hbm.at[0], w2),
    ]
    loads = [pltpu.make_async_copy(a, b, load_sem.at[n]) for n, (a, b) in enumerate(loads)]
    for load in loads:
        load.start()
    for load in loads[:3]:
        load.wait()

    lane = lax.broadcasted_iota(jnp.int32, (4, 128), 1)
    ids = routes[...]
    gates = fixed[...].astype(F32)
    weights = gates / jnp.sum(gates, axis=1, keepdims=True)
    names = jnp.zeros((4, 128), F32)
    weight = jnp.zeros((4, 128), F32)
    for k in range(ids.shape[1]):
        hit = ids[:, k : k + 1] == lane // CAP
        names = names + jnp.where(hit, 1.0, 0.0)
        weight = weight + jnp.where(hit, weights[:, k : k + 1], 0.0)
    before = [jnp.zeros((1, 128), F32)]
    for r in range(3):
        before.append(before[-1] + names[r : r + 1])
    before = jnp.concatenate(before, axis=0)
    selected = (names > 0.5) & (before == (lane % CAP).astype(F32))
    pick = jnp.where(selected, 1.0, 0.0)
    combine = jnp.where(selected, weight, 0.0)
    pick = jnp.concatenate([pick, jnp.zeros((4, 128), F32)], axis=0)
    pick = pick.T.astype(BF16)
    rows = tokens[...].astype(F32)
    rows = jnp.concatenate([rows, jnp.zeros_like(rows)], axis=0).astype(BF16)
    for j in range(jw):
        part = jnp.dot(pick, rows[:, j * 128 : (j + 1) * 128], preferred_element_type=F32)
        wide[pl.ds(j, ne * CAP, stride=jw), :] = part[: ne * CAP]
    for e in range(0, ne, 8):
        slots[e : e + 8] = wide[e * 16 : (e + 8) * 16, :].reshape(8, 16, 128).astype(BF16)

    c = Copies()
    pl.semaphore_wait(barrier, 2 * (nz - 1) + 5)

    gathered[h, 0, core] = slots[s]
    c.start(slots.at[z * 2 + 1 - core], gathered.at[h, 0, core], zs.at[1 - core], zr.at[core], chip(0, 1 - core))
    for i in range(1, nz):
        there = opposite(i, nz)
        for to in (0, 1):
            dev = chip(i, to)
            c.start(
                slots.at[dev[0]],
                gathered.at[h, there, core],
                zs.at[i * 2 + to],
                zr.at[there * 2 + core],
                dev,
            )

    for load in loads[3:]:
        load.wait()

    def grow(scale, count):
        v = scale[0].astype(F32)
        return jnp.concatenate(
            [jnp.broadcast_to(v[:, j : j + 1], (v.shape[0], 128)) for j in range(count)], axis=1
        )

    grown1[:, :f1] = grow(gs, f1 // QB)
    grown1[:, f1:] = grow(us, f1 // QB)
    grown2[...] = grow(ds_, dw // QB)

    def scale_w1(n, _):
        at = pl.ds(pl.multiple_of(n * 32, 32), 32)
        by = grown1[pl.ds(n // 4, 1), :]
        for half in (0, 1):
            cols = slice(half * f1, (half + 1) * f1)
            w1[at, cols] = (w1[at, cols].astype(F32) * by[:, cols]).astype(BF16)
        return 0

    def scale_w2(n, _):
        at = pl.ds(pl.multiple_of(n * 32, 32), 32)
        w2[at, :] = (w2[at, :].astype(F32) * grown2[pl.ds(n // 4, 1), :]).astype(BF16)
        return 0

    lax.fori_loop(0, w1.shape[0] // 32, scale_w1, 0)
    lax.fori_loop(0, w2.shape[0] // 32, scale_w2, 0)

    def span(k, part=None):
        if part is None:
            return pl.ds(k * ni, ni)
        return pl.ds(k * ni + part * (ni // 2), ni // 2)

    def recv(dst, sem, send=None):
        c.make(dst, dst, zs.at[0] if send is None else send, sem, dev_xr).wait_recv()

    def stage0(k):
        for i in range(k * ni, (k + 1) * ni):
            for frm in (0, 1):
                if i == 0:
                    continue
                recv(gathered.at[h, i, frm], zr.at[i * 2 + frm])
        if k == 0:
            recv(gathered.at[h, 0, 1 - core], zr.at[1 - core])
        block = gathered.at[h, span(k)]
        c.start(block, block, gx_s.at[k, 0], gx_r.at[k, 0], dev_xr)
        c.start(block, block, gx_s.at[k, 1], gx_r.at[k, 1], dev_xl)

    def stage1(k):
        recv(gathered.at[xl, span(k)], gx_r.at[k, 0])
        block = gathered.at[xl, span(k, 1)]
        c.start(block, block, gx_s.at[k, 2], gx_r.at[k, 2], dev_xr)
        recv(gathered.at[xr, span(k)], gx_r.at[k, 1])
        block = gathered.at[xr, span(k, 0)]
        c.start(block, block, gx_s.at[k, 3], gx_r.at[k, 3], dev_xl)

    def stage2(k):
        recv(gathered.at[xo, span(k, 1)], gx_r.at[k, 2])
        recv(gathered.at[xo, span(k, 0)], gx_r.at[k, 3])
        per = ni * 2 * 16
        for a in range(NX):
            wide[a * per : (a + 1) * per, :] = (
                gathered[a, k * ni : (k + 1) * ni].astype(F32).reshape(per, 128)
            )
        for j in range(jw):
            x_ref[:, j * 128 : (j + 1) * 128] = wide[pl.ds(j, m, stride=jw), :].astype(BF16)
        tiles = f1 // 256

        def tile(n, _):
            cols = pl.ds(pl.multiple_of(n * 256, 256), 256)
            part = jnp.dot(x_ref[...], w1[:, cols], preferred_element_type=F32)
            at = pl.ds(pl.multiple_of((n % tiles) * 256, 256), 256)
            partial[k, n // tiles, :, :, at] = part.reshape(NX, share, 256).astype(BF16)
            return 0

        lax.fori_loop(0, 2 * tiles, tile, 0)
        c.start(partial.at[k, 0, yo], relay_y.at[k, 0], ry_s.at[k, 0], ry_r.at[k, 0], dev_yr)
        c.start(partial.at[k, 1, yo], relay_y.at[k, 1], ry_s.at[k, 1], ry_r.at[k, 1], dev_yl)
        c.start(partial.at[k, 1, yr], arrive_y.at[k, 0, 1], ry_s.at[k, 2], ry_r.at[k, 2], dev_yr)
        c.start(partial.at[k, 0, yl], arrive_y.at[k, 1, 0], ry_s.at[k, 3], ry_r.at[k, 3], dev_yl)

    def stage3(k):
        recv(relay_y.at[k, 0], ry_r.at[k, 0])
        sums_y[k, 0] = (partial[k, 0, yr].astype(F32) + relay_y[k, 0].astype(F32)).astype(BF16)
        c.start(sums_y.at[k, 0], arrive_y.at[k, 0, 0], ry_s.at[k, 4], ry_r.at[k, 4], dev_yr)
        recv(relay_y.at[k, 1], ry_r.at[k, 1])
        sums_y[k, 1] = (partial[k, 1, yl].astype(F32) + relay_y[k, 1].astype(F32)).astype(BF16)
        c.start(sums_y.at[k, 1], arrive_y.at[k, 1, 1], ry_s.at[k, 5], ry_r.at[k, 5], dev_yl)

    def stage4(k):
        recv(arrive_y.at[k, 0, 1], ry_r.at[k, 2])
        recv(arrive_y.at[k, 1, 0], ry_r.at[k, 3])
        recv(arrive_y.at[k, 0, 0], ry_r.at[k, 4])
        recv(arrive_y.at[k, 1, 1], ry_r.at[k, 5])
        g, u = [
            partial[k, n, p].astype(F32) + arrive_y[k, 0, n].astype(F32) + arrive_y[k, 1, n].astype(F32)
            for n in (0, 1)
        ]
        hidden[k, p] = (g / (1.0 + jnp.exp(-g)) * u).astype(BF16)
        block = hidden.at[k, p]
        c.start(block, block, gy_s.at[k, 0], gy_r.at[k, 0], dev_yr)
        c.start(block, block, gy_s.at[k, 1], gy_r.at[k, 1], dev_yl)

    left, right = pl.ds(0, f1 // 2), pl.ds(f1 // 2, f1 // 2)

    def stage5(k):
        recv(hidden.at[k, yl], gy_r.at[k, 0])
        block = hidden.at[k, yl, :, left]
        c.start(block, block, gy_s.at[k, 2], gy_r.at[k, 2], dev_yr)
        recv(hidden.at[k, yr], gy_r.at[k, 1])
        block = hidden.at[k, yr, :, right]
        c.start(block, block, gy_s.at[k, 3], gy_r.at[k, 3], dev_yl)

    def stage6(k):
        recv(hidden.at[k, yo, :, left], gy_r.at[k, 2])
        recv(hidden.at[k, yo, :, right], gy_r.at[k, 3])
        tiles = dw // 512

        def tile(n, _):
            cols = pl.ds(pl.multiple_of(n * 256, 256), 256)
            act = hidden[k].reshape(m, f1)
            part = jnp.dot(act, w2[:, cols], preferred_element_type=F32)
            at = pl.ds(pl.multiple_of((n % tiles) * 256, 256), 256)
            outs[k, n // tiles, :, :, at] = part.reshape(NX, share, 256).astype(BF16)
            return 0

        lax.fori_loop(0, 2 * tiles, tile, 0)
        c.start(outs.at[k, 0, xo], relay_x.at[k, 0], rx_s.at[k, 0], rx_r.at[k, 0], dev_xr)
        c.start(outs.at[k, 1, xo], relay_x.at[k, 1], rx_s.at[k, 1], rx_r.at[k, 1], dev_xl)
        c.start(outs.at[k, 1, xr], arrive_x.at[k, 0, 1], rx_s.at[k, 2], rx_r.at[k, 2], dev_xr)
        c.start(outs.at[k, 0, xl], arrive_x.at[k, 1, 0], rx_s.at[k, 3], rx_r.at[k, 3], dev_xl)

    def stage7(k):
        recv(relay_x.at[k, 0], rx_r.at[k, 0])
        sums_x[k, 0] = (outs[k, 0, xr].astype(F32) + relay_x[k, 0].astype(F32)).astype(BF16)
        c.start(sums_x.at[k, 0], arrive_x.at[k, 0, 0], rx_s.at[k, 4], rx_r.at[k, 4], dev_xr)
        recv(relay_x.at[k, 1], rx_r.at[k, 1])
        sums_x[k, 1] = (outs[k, 1, xl].astype(F32) + relay_x[k, 1].astype(F32)).astype(BF16)
        c.start(sums_x.at[k, 1], arrive_x.at[k, 1, 1], rx_s.at[k, 5], rx_r.at[k, 5], dev_xl)

    def stage8(k):
        recv(arrive_x.at[k, 0, 1], rx_r.at[k, 2])
        recv(arrive_x.at[k, 1, 0], rx_r.at[k, 3])
        recv(arrive_x.at[k, 0, 0], rx_r.at[k, 4])
        recv(arrive_x.at[k, 1, 1], rx_r.at[k, 5])
        for n in (0, 1):
            y = outs[k, n, h].astype(F32) + arrive_x[k, 0, n].astype(F32) + arrive_x[k, 1, n].astype(F32)
            for j in range(jw // 2):
                back_wide[pl.ds(n * (jw // 2) + j, share, stride=jw), :] = y[:, j * 128 : (j + 1) * 128]
        back[k] = back_wide[...].reshape(ni, 2, 16, 128).astype(BF16)
        for n in reversed(range(ni)):
            i = k * ni + n
            for to in (0, 1):
                if i == 0:
                    continue
                there = opposite(i, nz)
                c.start(
                    back.at[k, n, to], results.at[s], bs.at[i * 2 + to], br.at[there * 2 + core], chip(i, to)
                )
        if k == 0:
            c.start(back.at[0, 0, 1 - core], results.at[s], bs.at[1 - core], br.at[core], chip(0, 1 - core))
            results[s] = back[0, 0, core]

    stages = [stage0, stage1, stage2, stage3, stage4, stage5, stage6, stage7, stage8]
    for t in range(len(stages) + nc - 1):
        for k in range(nc):
            if 0 <= t - k < len(stages):
                stages[t - k](k)

    for i, frm in peers:
        if i == 0:
            continue
        recv(results.at[chip(i, frm)[0]], br.at[i * 2 + frm])
    recv(results.at[z * 2 + 1 - core], br.at[1 - core])

    high = combine.astype(BF16).astype(F32)
    both = jnp.concatenate([high, combine - high], axis=0)[:, : ne * CAP].astype(BF16)
    for e in range(0, ne, 8):
        wide[e * 16 : (e + 8) * 16, :] = results[e : e + 8].astype(F32).reshape(128, 128)
    for j in range(jw):
        got = wide[pl.ds(j, ne * CAP, stride=jw), :].astype(BF16)
        part = jnp.dot(both, got, preferred_element_type=F32)
        out_ref[:, j * 128 : (j + 1) * 128] = (part[:4] + part[4:]).astype(BF16)
    for copy in c.sent:
        copy.wait_send()


def solution(mesh):
    nz = mesh.shape["seq"] // 2

    def step(*args):
        tokens, routes, fixed, gate, _, down, gs, us, ds_ = args
        dw, f1 = gate.shape[1:]
        nc, ni = CHUNKS, nz // CHUNKS
        m = NX * ni * 2 * CAP
        share = m // NX
        ne = 2 * nz
        dma = pltpu.SemaphoreType.DMA
        scratch = [
            pltpu.VMEM(tokens.shape, BF16),
            pltpu.VMEM(routes.shape, jnp.int32),
            pltpu.VMEM(fixed.shape, jnp.int32),
            pltpu.VMEM((dw, 2 * f1), BF16),
            pltpu.VMEM((f1, dw), BF16),
            pltpu.VMEM(gs.shape, BF16),
            pltpu.VMEM(us.shape, BF16),
            pltpu.VMEM(ds_.shape, BF16),
            pltpu.VMEM((dw // QB, 2 * f1), F32),
            pltpu.VMEM((f1 // QB, dw), F32),
            pltpu.VMEM((ne, 16, 128), BF16),
            pltpu.VMEM((NX, nz, 2, 16, 128), BF16),
            pltpu.VMEM((max(m, ne * CAP) * 8, 128), F32),
            pltpu.VMEM((m, dw), BF16),
            pltpu.VMEM((nc, 2, NX, share, f1), BF16),
            pltpu.VMEM((nc, 2, share, f1), BF16),
            pltpu.VMEM((nc, 2, share, f1), BF16),
            pltpu.VMEM((nc, 2, 2, share, f1), BF16),
            pltpu.VMEM((nc, NX, share, f1), BF16),
            pltpu.VMEM((nc, 2, NX, share, dw // 2), BF16),
            pltpu.VMEM((nc, 2, share, dw // 2), BF16),
            pltpu.VMEM((nc, 2, share, dw // 2), BF16),
            pltpu.VMEM((nc, 2, 2, share, dw // 2), BF16),
            pltpu.VMEM((share * 8, 128), F32),
            pltpu.VMEM((nc, ni, 2, 16, 128), BF16),
            pltpu.VMEM((ne, 16, 128), BF16),
            dma((9,)),
            dma((2 * nz,)),
            dma((2 * nz,)),
            dma((nc, 4)),
            dma((nc, 4)),
            dma((nc, 6)),
            dma((nc, 6)),
            dma((nc, 4)),
            dma((nc, 4)),
            dma((nc, 6)),
            dma((nc, 6)),
            dma((2 * nz,)),
            dma((2 * nz,)),
        ]
        return pl.pallas_call(
            functools.partial(kernel, nz),
            out_shape=jax.ShapeDtypeStruct(tokens.shape, BF16),
            in_specs=[pl.BlockSpec(memory_space=pl.ANY)] * 9,
            out_specs=pl.BlockSpec(memory_space=pltpu.VMEM),
            scratch_shapes=scratch,
            compiler_params=pltpu.CompilerParams(
                collective_id=0, has_side_effects=True, vmem_limit_bytes=40 * 1024 * 1024
            ),
        )(*args)

    return jax.shard_map(
        step,
        mesh=mesh,
        in_specs=(
            P(("seq", "head"), "pool"),
            P(("seq", "head"), None),
            P(("seq", "head"), None),
            P("seq", "pool", "head"),
            P("seq", "pool", "head"),
            P("seq", "head", "pool"),
            P("seq", "pool", "head"),
            P("seq", "pool", "head"),
            P("seq", "head", "pool"),
        ),
        out_specs=P(("seq", "head"), "pool"),
        check_vma=False,
    )
```

```python
import functools

import jax
import jax.numpy as jnp
from jax import lax
from jax.experimental import pallas as pl
from jax.experimental.pallas import tpu as pltpu
from jax.sharding import PartitionSpec as P

QB = 128
CAP = 2
NX = 4
CHUNKS = 2
F32 = jnp.float32
BF16 = jnp.bfloat16


def offset(i):
    k = (i + 1) // 2
    return k if i % 2 == 0 else -k


def opposite(i, nz):
    if i == 0:
        return 0
    other = i + 1 if i % 2 else i - 1
    return other if other < nz else i


class Copies:
    def __init__(self):
        self.sent = []

    def make(self, src, dst, send, recv, device):
        return pltpu.make_async_remote_copy(
            src_ref=src,
            dst_ref=dst,
            send_sem=send,
            recv_sem=recv,
            device_id=device,
            device_id_type=pl.DeviceIdType.MESH,
        )

    def start(self, *args):
        copy = self.make(*args)
        copy.start()
        self.sent.append(copy)


def kernel(
    nz,
    tokens_hbm,
    routes_hbm,
    fixed_hbm,
    gate_hbm,
    up_hbm,
    down_hbm,
    gs_hbm,
    us_hbm,
    ds_hbm,
    out_ref,
    tokens,
    routes,
    fixed,
    w1,
    w2,
    gs,
    us,
    ds_,
    grown1,
    grown2,
    slots,
    gathered,
    wide,
    x_ref,
    partial,
    relay_y,
    sums_y,
    arrive_y,
    hidden,
    outs,
    relay_x,
    sums_x,
    arrive_x,
    back_wide,
    back,
    results,
    load_sem,
    zs,
    zr,
    gx_s,
    gx_r,
    ry_s,
    ry_r,
    gy_s,
    gy_r,
    rx_s,
    rx_r,
    bs,
    br,
):
    s = lax.axis_index("seq")
    h = lax.axis_index("head")
    p = lax.axis_index("pool")
    z = s // 2
    core = s % 2
    nc = CHUNKS
    ni = nz // nc
    ne = 2 * nz
    m = NX * ni * 2 * CAP
    share = m // NX
    f1 = w1.shape[1] // 2
    dw = w2.shape[1]
    jw = dw // 128

    def near(base, step):
        return (base + step + NX) % NX

    xr, xl, xo = near(h, 1), near(h, -1), near(h, 2)
    yr, yl, yo = near(p, 1), near(p, -1), near(p, 2)
    dev_xr, dev_xl = (s, xr, p), (s, xl, p)
    dev_yr, dev_yl = (s, h, yr), (s, h, yl)

    def chip(i, to_core):
        return (((z + offset(i) + nz) % nz) * 2 + to_core, h, p)

    peers = [(i, c) for i in range(nz) for c in (0, 1)]

    barrier = pltpu.get_barrier_semaphore()
    for i in range(nz - 1, 0, -1):
        for c in (0, 1):
            pl.semaphore_signal(barrier, inc=1, device_id=chip(i, c), device_id_type=pl.DeviceIdType.MESH)
    for dev in (chip(0, 1 - core), dev_xr, dev_xl, dev_yr, dev_yl):
        pl.semaphore_signal(barrier, inc=1, device_id=dev, device_id_type=pl.DeviceIdType.MESH)

    loads = [
        (tokens_hbm, tokens),
        (routes_hbm, routes),
        (fixed_hbm, fixed),
        (gs_hbm, gs),
        (us_hbm, us),
        (ds_hbm, ds_),
        (gate_hbm.at[0], w1.at[:, pl.ds(0, f1)]),
        (up_hbm.at[0], w1.at[:, pl.ds(f1, f1)]),
        (down_hbm.at[0], w2),
    ]
    loads = [pltpu.make_async_copy(a, b, load_sem.at[n]) for n, (a, b) in enumerate(loads)]
    for load in loads:
        load.start()
    for load in loads[:3]:
        load.wait()

    lane = lax.broadcasted_iota(jnp.int32, (4, 128), 1)
    ids = routes[...]
    gates = fixed[...].astype(F32)
    weights = gates / jnp.sum(gates, axis=1, keepdims=True)
    names = jnp.zeros((4, 128), F32)
    weight = jnp.zeros((4, 128), F32)
    for k in range(ids.shape[1]):
        hit = ids[:, k : k + 1] == lane // CAP
        names = names + jnp.where(hit, 1.0, 0.0)
        weight = weight + jnp.where(hit, weights[:, k : k + 1], 0.0)
    before = [jnp.zeros((1, 128), F32)]
    for r in range(3):
        before.append(before[-1] + names[r : r + 1])
    before = jnp.concatenate(before, axis=0)
    selected = (names > 0.5) & (before == (lane % CAP).astype(F32))
    pick = jnp.where(selected, 1.0, 0.0)
    combine = jnp.where(selected, weight, 0.0)
    pick = jnp.concatenate([pick, jnp.zeros((4, 128), F32)], axis=0)
    pick = pick.T.astype(BF16)
    rows = tokens[...].astype(F32)
    rows = jnp.concatenate([rows, jnp.zeros_like(rows)], axis=0).astype(BF16)
    for j in range(jw):
        part = jnp.dot(pick, rows[:, j * 128 : (j + 1) * 128], preferred_element_type=F32)
        wide[pl.ds(j, ne * CAP, stride=jw), :] = part[: ne * CAP]
    for e in range(0, ne, 8):
        slots[e : e + 8] = wide[e * 16 : (e + 8) * 16, :].reshape(8, 16, 128).astype(BF16)

    c = Copies()
    with jax.named_scope("greet"):
        pl.semaphore_wait(barrier, 2 * (nz - 1) + 5)

    gathered[h, 0, core] = slots[s]
    c.start(slots.at[z * 2 + 1 - core], gathered.at[h, 0, core], zs.at[1 - core], zr.at[core], chip(0, 1 - core))
    for i in range(1, nz):
        there = opposite(i, nz)
        for to in (0, 1):
            dev = chip(i, to)
            c.start(
                slots.at[dev[0]],
                gathered.at[h, there, core],
                zs.at[i * 2 + to],
                zr.at[there * 2 + core],
                dev,
            )

    with jax.named_scope("loads"):
        for load in loads[3:]:
            load.wait()

    def grow(scale, count):
        v = scale[0].astype(F32)
        return jnp.concatenate(
            [jnp.broadcast_to(v[:, j : j + 1], (v.shape[0], 128)) for j in range(count)], axis=1
        )

    grown1[:, :f1] = grow(gs, f1 // QB)
    grown1[:, f1:] = grow(us, f1 // QB)
    grown2[...] = grow(ds_, dw // QB)

    def scale_w1(n, _):
        at = pl.ds(pl.multiple_of(n * 32, 32), 32)
        by = grown1[pl.ds(n // 4, 1), :]
        for half in (0, 1):
            cols = slice(half * f1, (half + 1) * f1)
            w1[at, cols] = (w1[at, cols].astype(F32) * by[:, cols]).astype(BF16)
        return 0

    def scale_w2(n, _):
        at = pl.ds(pl.multiple_of(n * 32, 32), 32)
        w2[at, :] = (w2[at, :].astype(F32) * grown2[pl.ds(n // 4, 1), :]).astype(BF16)
        return 0

    with jax.named_scope("scale"):
        lax.fori_loop(0, w1.shape[0] // 32, scale_w1, 0)
        lax.fori_loop(0, w2.shape[0] // 32, scale_w2, 0)

    def span(k, part=None):
        if part is None:
            return pl.ds(k * ni, ni)
        return pl.ds(k * ni + part * (ni // 2), ni // 2)

    def recv(dst, sem, send=None):
        c.make(dst, dst, zs.at[0] if send is None else send, sem, dev_xr).wait_recv()

    def stage0(k):
        for i in range(k * ni, (k + 1) * ni):
            for frm in (0, 1):
                if i == 0:
                    continue
                recv(gathered.at[h, i, frm], zr.at[i * 2 + frm])
        if k == 0:
            recv(gathered.at[h, 0, 1 - core], zr.at[1 - core])
        block = gathered.at[h, span(k)]
        c.start(block, block, gx_s.at[k, 0], gx_r.at[k, 0], dev_xr)
        c.start(block, block, gx_s.at[k, 1], gx_r.at[k, 1], dev_xl)

    def stage1(k):
        recv(gathered.at[xl, span(k)], gx_r.at[k, 0])
        block = gathered.at[xl, span(k, 1)]
        c.start(block, block, gx_s.at[k, 2], gx_r.at[k, 2], dev_xr)
        recv(gathered.at[xr, span(k)], gx_r.at[k, 1])
        block = gathered.at[xr, span(k, 0)]
        c.start(block, block, gx_s.at[k, 3], gx_r.at[k, 3], dev_xl)

    def stage2(k):
        recv(gathered.at[xo, span(k, 1)], gx_r.at[k, 2])
        recv(gathered.at[xo, span(k, 0)], gx_r.at[k, 3])
        per = ni * 2 * 16
        for a in range(NX):
            wide[a * per : (a + 1) * per, :] = (
                gathered[a, k * ni : (k + 1) * ni].astype(F32).reshape(per, 128)
            )
        for j in range(jw):
            x_ref[:, j * 128 : (j + 1) * 128] = wide[pl.ds(j, m, stride=jw), :].astype(BF16)
        tiles = f1 // 256

        def tile(n, _):
            cols = pl.ds(pl.multiple_of(n * 256, 256), 256)
            part = jnp.dot(x_ref[...], w1[:, cols], preferred_element_type=F32)
            at = pl.ds(pl.multiple_of((n % tiles) * 256, 256), 256)
            partial[k, n // tiles, :, :, at] = part.reshape(NX, share, 256).astype(BF16)
            return 0

        lax.fori_loop(0, 2 * tiles, tile, 0)
        c.start(partial.at[k, 0, yo], relay_y.at[k, 0], ry_s.at[k, 0], ry_r.at[k, 0], dev_yr)
        c.start(partial.at[k, 1, yo], relay_y.at[k, 1], ry_s.at[k, 1], ry_r.at[k, 1], dev_yl)
        c.start(partial.at[k, 1, yr], arrive_y.at[k, 0, 1], ry_s.at[k, 2], ry_r.at[k, 2], dev_yr)
        c.start(partial.at[k, 0, yl], arrive_y.at[k, 1, 0], ry_s.at[k, 3], ry_r.at[k, 3], dev_yl)

    def stage3(k):
        recv(relay_y.at[k, 0], ry_r.at[k, 0])
        sums_y[k, 0] = (partial[k, 0, yr].astype(F32) + relay_y[k, 0].astype(F32)).astype(BF16)
        c.start(sums_y.at[k, 0], arrive_y.at[k, 0, 0], ry_s.at[k, 4], ry_r.at[k, 4], dev_yr)
        recv(relay_y.at[k, 1], ry_r.at[k, 1])
        sums_y[k, 1] = (partial[k, 1, yl].astype(F32) + relay_y[k, 1].astype(F32)).astype(BF16)
        c.start(sums_y.at[k, 1], arrive_y.at[k, 1, 1], ry_s.at[k, 5], ry_r.at[k, 5], dev_yl)

    def stage4(k):
        recv(arrive_y.at[k, 0, 1], ry_r.at[k, 2])
        recv(arrive_y.at[k, 1, 0], ry_r.at[k, 3])
        recv(arrive_y.at[k, 0, 0], ry_r.at[k, 4])
        recv(arrive_y.at[k, 1, 1], ry_r.at[k, 5])
        g, u = [
            partial[k, n, p].astype(F32) + arrive_y[k, 0, n].astype(F32) + arrive_y[k, 1, n].astype(F32)
            for n in (0, 1)
        ]
        hidden[k, p] = (g / (1.0 + jnp.exp(-g)) * u).astype(BF16)
        block = hidden.at[k, p]
        c.start(block, block, gy_s.at[k, 0], gy_r.at[k, 0], dev_yr)
        c.start(block, block, gy_s.at[k, 1], gy_r.at[k, 1], dev_yl)

    left, right = pl.ds(0, f1 // 2), pl.ds(f1 // 2, f1 // 2)

    def stage5(k):
        recv(hidden.at[k, yl], gy_r.at[k, 0])
        block = hidden.at[k, yl, :, left]
        c.start(block, block, gy_s.at[k, 2], gy_r.at[k, 2], dev_yr)
        recv(hidden.at[k, yr], gy_r.at[k, 1])
        block = hidden.at[k, yr, :, right]
        c.start(block, block, gy_s.at[k, 3], gy_r.at[k, 3], dev_yl)

    def stage6(k):
        recv(hidden.at[k, yo, :, left], gy_r.at[k, 2])
        recv(hidden.at[k, yo, :, right], gy_r.at[k, 3])
        tiles = dw // 512

        def tile(n, _):
            cols = pl.ds(pl.multiple_of(n * 256, 256), 256)
            act = hidden[k].reshape(m, f1)
            part = jnp.dot(act, w2[:, cols], preferred_element_type=F32)
            at = pl.ds(pl.multiple_of((n % tiles) * 256, 256), 256)
            outs[k, n // tiles, :, :, at] = part.reshape(NX, share, 256).astype(BF16)
            return 0

        lax.fori_loop(0, 2 * tiles, tile, 0)
        c.start(outs.at[k, 0, xo], relay_x.at[k, 0], rx_s.at[k, 0], rx_r.at[k, 0], dev_xr)
        c.start(outs.at[k, 1, xo], relay_x.at[k, 1], rx_s.at[k, 1], rx_r.at[k, 1], dev_xl)
        c.start(outs.at[k, 1, xr], arrive_x.at[k, 0, 1], rx_s.at[k, 2], rx_r.at[k, 2], dev_xr)
        c.start(outs.at[k, 0, xl], arrive_x.at[k, 1, 0], rx_s.at[k, 3], rx_r.at[k, 3], dev_xl)

    def stage7(k):
        recv(relay_x.at[k, 0], rx_r.at[k, 0])
        sums_x[k, 0] = (outs[k, 0, xr].astype(F32) + relay_x[k, 0].astype(F32)).astype(BF16)
        c.start(sums_x.at[k, 0], arrive_x.at[k, 0, 0], rx_s.at[k, 4], rx_r.at[k, 4], dev_xr)
        recv(relay_x.at[k, 1], rx_r.at[k, 1])
        sums_x[k, 1] = (outs[k, 1, xl].astype(F32) + relay_x[k, 1].astype(F32)).astype(BF16)
        c.start(sums_x.at[k, 1], arrive_x.at[k, 1, 1], rx_s.at[k, 5], rx_r.at[k, 5], dev_xl)

    def stage8(k):
        recv(arrive_x.at[k, 0, 1], rx_r.at[k, 2])
        recv(arrive_x.at[k, 1, 0], rx_r.at[k, 3])
        recv(arrive_x.at[k, 0, 0], rx_r.at[k, 4])
        recv(arrive_x.at[k, 1, 1], rx_r.at[k, 5])
        for n in (0, 1):
            y = outs[k, n, h].astype(F32) + arrive_x[k, 0, n].astype(F32) + arrive_x[k, 1, n].astype(F32)
            for j in range(jw // 2):
                back_wide[pl.ds(n * (jw // 2) + j, share, stride=jw), :] = y[:, j * 128 : (j + 1) * 128]
        back[k] = back_wide[...].reshape(ni, 2, 16, 128).astype(BF16)
        for n in reversed(range(ni)):
            i = k * ni + n
            for to in (0, 1):
                if i == 0:
                    continue
                there = opposite(i, nz)
                c.start(
                    back.at[k, n, to], results.at[s], bs.at[i * 2 + to], br.at[there * 2 + core], chip(i, to)
                )
        if k == 0:
            c.start(back.at[0, 0, 1 - core], results.at[s], bs.at[1 - core], br.at[core], chip(0, 1 - core))
            results[s] = back[0, 0, core]

    stages = [stage0, stage1, stage2, stage3, stage4, stage5, stage6, stage7, stage8]
    for t in range(len(stages) + nc - 1):
        for k in range(nc):
            if 0 <= t - k < len(stages):
                with jax.named_scope(f"s{t - k}c{k}"):
                    stages[t - k](k)

    with jax.named_scope("back"):
        for i, frm in peers:
            if i == 0:
                continue
            recv(results.at[chip(i, frm)[0]], br.at[i * 2 + frm])
        recv(results.at[z * 2 + 1 - core], br.at[1 - core])

    high = combine.astype(BF16).astype(F32)
    both = jnp.concatenate([high, combine - high], axis=0)[:, : ne * CAP].astype(BF16)
    for e in range(0, ne, 8):
        wide[e * 16 : (e + 8) * 16, :] = results[e : e + 8].astype(F32).reshape(128, 128)
    for j in range(jw):
        got = wide[pl.ds(j, ne * CAP, stride=jw), :].astype(BF16)
        part = jnp.dot(both, got, preferred_element_type=F32)
        out_ref[:, j * 128 : (j + 1) * 128] = (part[:4] + part[4:]).astype(BF16)
    for copy in c.sent:
        copy.wait_send()


def solution(mesh):
    nz = mesh.shape["seq"] // 2

    def step(*args):
        tokens, routes, fixed, gate, _, down, gs, us, ds_ = args
        dw, f1 = gate.shape[1:]
        nc, ni = CHUNKS, nz // CHUNKS
        m = NX * ni * 2 * CAP
        share = m // NX
        ne = 2 * nz
        dma = pltpu.SemaphoreType.DMA
        scratch = [
            pltpu.VMEM(tokens.shape, BF16),
            pltpu.VMEM(routes.shape, jnp.int32),
            pltpu.VMEM(fixed.shape, jnp.int32),
            pltpu.VMEM((dw, 2 * f1), BF16),
            pltpu.VMEM((f1, dw), BF16),
            pltpu.VMEM(gs.shape, BF16),
            pltpu.VMEM(us.shape, BF16),
            pltpu.VMEM(ds_.shape, BF16),
            pltpu.VMEM((dw // QB, 2 * f1), F32),
            pltpu.VMEM((f1 // QB, dw), F32),
            pltpu.VMEM((ne, 16, 128), BF16),
            pltpu.VMEM((NX, nz, 2, 16, 128), BF16),
            pltpu.VMEM((max(m, ne * CAP) * 8, 128), F32),
            pltpu.VMEM((m, dw), BF16),
            pltpu.VMEM((nc, 2, NX, share, f1), BF16),
            pltpu.VMEM((nc, 2, share, f1), BF16),
            pltpu.VMEM((nc, 2, share, f1), BF16),
            pltpu.VMEM((nc, 2, 2, share, f1), BF16),
            pltpu.VMEM((nc, NX, share, f1), BF16),
            pltpu.VMEM((nc, 2, NX, share, dw // 2), BF16),
            pltpu.VMEM((nc, 2, share, dw // 2), BF16),
            pltpu.VMEM((nc, 2, share, dw // 2), BF16),
            pltpu.VMEM((nc, 2, 2, share, dw // 2), BF16),
            pltpu.VMEM((share * 8, 128), F32),
            pltpu.VMEM((nc, ni, 2, 16, 128), BF16),
            pltpu.VMEM((ne, 16, 128), BF16),
            dma((9,)),
            dma((2 * nz,)),
            dma((2 * nz,)),
            dma((nc, 4)),
            dma((nc, 4)),
            dma((nc, 6)),
            dma((nc, 6)),
            dma((nc, 4)),
            dma((nc, 4)),
            dma((nc, 6)),
            dma((nc, 6)),
            dma((2 * nz,)),
            dma((2 * nz,)),
        ]
        return pl.pallas_call(
            functools.partial(kernel, nz),
            out_shape=jax.ShapeDtypeStruct(tokens.shape, BF16),
            in_specs=[pl.BlockSpec(memory_space=pltpu.HBM)] * 9,
            out_specs=pl.BlockSpec(memory_space=pltpu.VMEM),
            scratch_shapes=scratch,
            compiler_params=pltpu.CompilerParams(
                collective_id=0, has_side_effects=True, vmem_limit_bytes=60 * 1024 * 1024
            ),
        )(*args)

    return jax.shard_map(
        step,
        mesh=mesh,
        in_specs=(
            P(("seq", "head"), "pool"),
            P(("seq", "head"), None),
            P(("seq", "head"), None),
            P("seq", "pool", "head"),
            P("seq", "pool", "head"),
            P("seq", "head", "pool"),
            P("seq", "pool", "head"),
            P("seq", "pool", "head"),
            P("seq", "head", "pool"),
        ),
        out_specs=P(("seq", "head"), "pool"),
        check_vma=False,
    )
```

```python
import functools

import jax
import jax.numpy as jnp
from jax import lax
from jax.experimental import pallas as pl
from jax.experimental.pallas import tpu as pltpu
from jax.sharding import PartitionSpec as P

QB = 128
CAP = 2
NX = 4
CHUNKS = 4
ORDER = [divmod(n, 10) for n in (0, 1, 2, 10, 3, 11, 12, 20, 13, 21, 22, 30, 23, 31, 32, 40, 33, 41, 42, 43)]
F32 = jnp.float32
BF16 = jnp.bfloat16


def offset(i):
    k = (i + 1) // 2
    return k if i % 2 == 0 else -k


def opposite(i, nz):
    if i == 0:
        return 0
    other = i + 1 if i % 2 else i - 1
    return other if other < nz else i


class Copies:
    def __init__(self):
        self.sent = []

    def make(self, src, dst, send, recv, device):
        return pltpu.make_async_remote_copy(
            src_ref=src,
            dst_ref=dst,
            send_sem=send,
            recv_sem=recv,
            device_id=device,
            device_id_type=pl.DeviceIdType.MESH,
        )

    def start(self, *args):
        copy = self.make(*args)
        copy.start()
        self.sent.append(copy)


def kernel(
    nz,
    tokens_hbm,
    routes_hbm,
    fixed_hbm,
    gate_hbm,
    up_hbm,
    down_hbm,
    gs_hbm,
    us_hbm,
    ds_hbm,
    out_ref,
    tokens,
    routes,
    fixed,
    w1,
    w2,
    gs,
    us,
    ds_,
    grown1,
    grown2,
    slots,
    gathered,
    wide,
    x_ref,
    partial,
    arrive_y,
    hidden,
    outs,
    arrive_x,
    back_wide,
    back,
    results,
    load_sem,
    zs,
    zr,
    gx_s,
    gx_r,
    ry_s,
    ry_r,
    gy_s,
    gy_r,
    rx_s,
    rx_r,
    bs,
    br,
):
    s = lax.axis_index("seq")
    h = lax.axis_index("head")
    p = lax.axis_index("pool")
    z = s // 2
    core = s % 2
    nc = CHUNKS
    ni = nz // nc
    ne = 2 * nz
    m = NX * ni * 2 * CAP
    share = m // NX
    f1 = w1.shape[1] // 2
    dw = w2.shape[1]
    jw = dw // 128

    def near(base, step):
        return (base + step + NX) % NX

    xr, xl, xo = near(h, 1), near(h, -1), near(h, 2)
    yr, yl, yo = near(p, 1), near(p, -1), near(p, 2)
    devs_x = [(s, a, p) for a in (xo, xr, xl)]
    devs_y = [(s, h, a) for a in (yo, yr, yl)]

    def chip(i, to_core):
        return (((z + offset(i) + nz) % nz) * 2 + to_core, h, p)

    peers = [(i, c) for i in range(nz) for c in (0, 1)]

    barrier = pltpu.get_barrier_semaphore()
    for i in range(nz - 1, 0, -1):
        for c in (0, 1):
            pl.semaphore_signal(barrier, inc=1, device_id=chip(i, c), device_id_type=pl.DeviceIdType.MESH)
    for dev in (chip(0, 1 - core), *devs_x, *devs_y):
        pl.semaphore_signal(barrier, inc=1, device_id=dev, device_id_type=pl.DeviceIdType.MESH)

    loads = [
        (tokens_hbm, tokens),
        (routes_hbm, routes),
        (fixed_hbm, fixed),
        (gs_hbm, gs),
        (us_hbm, us),
        (ds_hbm, ds_),
        (gate_hbm.at[0], w1.at[:, pl.ds(0, f1)]),
        (up_hbm.at[0], w1.at[:, pl.ds(f1, f1)]),
        (down_hbm.at[0], w2),
    ]
    loads = [pltpu.make_async_copy(a, b, load_sem.at[n]) for n, (a, b) in enumerate(loads)]
    for load in loads:
        load.start()
    for load in loads[:3]:
        load.wait()

    lane = lax.broadcasted_iota(jnp.int32, (4, 128), 1)
    ids = routes[...]
    gates = fixed[...].astype(F32)
    weights = gates / jnp.sum(gates, axis=1, keepdims=True)
    names = jnp.zeros((4, 128), F32)
    weight = jnp.zeros((4, 128), F32)
    for k in range(ids.shape[1]):
        hit = ids[:, k : k + 1] == lane // CAP
        names = names + jnp.where(hit, 1.0, 0.0)
        weight = weight + jnp.where(hit, weights[:, k : k + 1], 0.0)
    before = [jnp.zeros((1, 128), F32)]
    for r in range(3):
        before.append(before[-1] + names[r : r + 1])
    before = jnp.concatenate(before, axis=0)
    selected = (names > 0.5) & (before == (lane % CAP).astype(F32))
    pick = jnp.where(selected, 1.0, 0.0)
    combine = jnp.where(selected, weight, 0.0)
    pick = jnp.concatenate([pick, jnp.zeros((4, 128), F32)], axis=0)
    pick = pick.T.astype(BF16)
    rows = tokens[...].astype(F32)
    rows = jnp.concatenate([rows, jnp.zeros_like(rows)], axis=0).astype(BF16)
    for j in range(jw):
        part = jnp.dot(pick, rows[:, j * 128 : (j + 1) * 128], preferred_element_type=F32)
        wide[pl.ds(j, ne * CAP, stride=jw), :] = part[: ne * CAP]
    for e in range(0, ne, 8):
        slots[e : e + 8] = wide[e * 16 : (e + 8) * 16, :].reshape(8, 16, 128).astype(BF16)

    c = Copies()
    with jax.named_scope("greet"):
        pl.semaphore_wait(barrier, 2 * (nz - 1) + 7)

    gathered[h, 0, core] = slots[s]
    c.start(slots.at[z * 2 + 1 - core], gathered.at[h, 0, core], zs.at[1 - core], zr.at[core], chip(0, 1 - core))
    for i in range(1, nz):
        there = opposite(i, nz)
        for to in (0, 1):
            dev = chip(i, to)
            c.start(
                slots.at[dev[0]],
                gathered.at[h, there, core],
                zs.at[i * 2 + to],
                zr.at[there * 2 + core],
                dev,
            )

    with jax.named_scope("loads"):
        for load in loads[3:]:
            load.wait()

    def grow(scale, count):
        v = scale[0].astype(F32)
        return jnp.concatenate(
            [jnp.broadcast_to(v[:, j : j + 1], (v.shape[0], 128)) for j in range(count)], axis=1
        )

    grown1[:, :f1] = grow(gs, f1 // QB)
    grown1[:, f1:] = grow(us, f1 // QB)
    grown2[...] = grow(ds_, dw // QB)

    def scale_w1(n, _):
        at = pl.ds(pl.multiple_of(n * 32, 32), 32)
        by = grown1[pl.ds(n // 4, 1), :]
        for half in (0, 1):
            cols = slice(half * f1, (half + 1) * f1)
            w1[at, cols] = (w1[at, cols].astype(F32) * by[:, cols]).astype(BF16)
        return 0

    def scale_w2(n, _):
        at = pl.ds(pl.multiple_of(n * 32, 32), 32)
        w2[at, :] = (w2[at, :].astype(F32) * grown2[pl.ds(n // 4, 1), :]).astype(BF16)
        return 0

    with jax.named_scope("scale"):
        lax.fori_loop(0, w1.shape[0] // 32, scale_w1, 0)
        lax.fori_loop(0, w2.shape[0] // 32, scale_w2, 0)

    def span(k):
        return pl.ds(k * ni, ni)

    def recv(dst, sem):
        c.make(dst, dst, zs.at[0], sem, devs_x[0]).wait_recv()

    def stage0(k):
        for i in range(k * ni, (k + 1) * ni):
            for frm in (0, 1):
                if i == 0:
                    continue
                recv(gathered.at[h, i, frm], zr.at[i * 2 + frm])
        if k == 0:
            recv(gathered.at[h, 0, 1 - core], zr.at[1 - core])
        block = gathered.at[h, span(k)]
        for n, dev in enumerate(devs_x):
            c.start(block, block, gx_s.at[k, n], gx_r.at[k, n], dev)

    def stage1(k):
        per = ni * 2 * 16
        for n, a in enumerate((xo, xl, xr)):
            recv(gathered.at[a, span(k)], gx_r.at[k, n])
        for a in range(NX):
            wide[a * per : (a + 1) * per, :] = (
                gathered[a, k * ni : (k + 1) * ni].astype(F32).reshape(per, 128)
            )
        for j in range(jw):
            x_ref[:, j * 128 : (j + 1) * 128] = wide[pl.ds(j, m, stride=jw), :].astype(BF16)
        tiles = f1 // 256

        def tile(n, _):
            cols = pl.ds(pl.multiple_of(n * 256, 256), 256)
            part = jnp.dot(x_ref[...], w1[:, cols], preferred_element_type=F32)
            at = pl.ds(pl.multiple_of((n % tiles) * 256, 256), 256)
            partial[k, n // tiles, :, :, at] = part.reshape(NX, share, 256).astype(BF16)
            return 0

        for half in (0, 1):
            lax.fori_loop(half * tiles, (half + 1) * tiles, tile, 0)
            for n, (to, dev) in enumerate(zip((yo, yr, yl), devs_y)):
                c.start(
                    partial.at[k, half, to],
                    arrive_y.at[k, n, half],
                    ry_s.at[k, half * 3 + n],
                    ry_r.at[k, half * 3 + n],
                    dev,
                )

    def total(mine, arrived, k, half):
        return mine.astype(F32) + (
            arrived[k, 0, half].astype(F32) + arrived[k, 1, half].astype(F32) + arrived[k, 2, half].astype(F32)
        )

    def stage2(k):
        for half in (0, 1):
            for n in range(3):
                recv(arrive_y.at[k, n, half], ry_r.at[k, half * 3 + n])
        g = total(partial[k, 0, p], arrive_y, k, 0)
        u = total(partial[k, 1, p], arrive_y, k, 1)
        hidden[k, p] = (g / (1.0 + jnp.exp(-g)) * u).astype(BF16)
        block = hidden.at[k, p]
        for n, dev in enumerate(devs_y):
            c.start(block, block, gy_s.at[k, n], gy_r.at[k, n], dev)

    def stage3(k):
        for n, a in enumerate((yo, yl, yr)):
            recv(hidden.at[k, a], gy_r.at[k, n])
        tiles = dw // 512

        def tile(n, _):
            cols = pl.ds(pl.multiple_of(n * 256, 256), 256)
            act = hidden[k].reshape(m, f1)
            part = jnp.dot(act, w2[:, cols], preferred_element_type=F32)
            at = pl.ds(pl.multiple_of((n % tiles) * 256, 256), 256)
            outs[k, n // tiles, :, :, at] = part.reshape(NX, share, 256).astype(BF16)
            return 0

        for half in (0, 1):
            lax.fori_loop(half * tiles, (half + 1) * tiles, tile, 0)
            for n, (to, dev) in enumerate(zip((xo, xr, xl), devs_x)):
                c.start(
                    outs.at[k, half, to],
                    arrive_x.at[k, n, half],
                    rx_s.at[k, half * 3 + n],
                    rx_r.at[k, half * 3 + n],
                    dev,
                )

    def stage4(k):
        for half in (0, 1):
            for n in range(3):
                recv(arrive_x.at[k, n, half], rx_r.at[k, half * 3 + n])
        for n in (0, 1):
            y = total(outs[k, n, h], arrive_x, k, n)
            for j in range(jw // 2):
                back_wide[pl.ds(n * (jw // 2) + j, share, stride=jw), :] = y[:, j * 128 : (j + 1) * 128]
        back[k] = back_wide[...].reshape(ni, 2, 16, 128).astype(BF16)
        for n in reversed(range(ni)):
            i = k * ni + n
            for to in (0, 1):
                if i == 0:
                    continue
                there = opposite(i, nz)
                c.start(
                    back.at[k, n, to], results.at[s], bs.at[i * 2 + to], br.at[there * 2 + core], chip(i, to)
                )
        if k == 0:
            c.start(back.at[0, 0, 1 - core], results.at[s], bs.at[1 - core], br.at[core], chip(0, 1 - core))
            results[s] = back[0, 0, core]

    stages = [stage0, stage1, stage2, stage3, stage4]
    for n, k in ORDER:
        with jax.named_scope(f"s{n}c{k}"):
            stages[n](k)

    with jax.named_scope("back"):
        for i, frm in peers:
            if i == 0:
                continue
            recv(results.at[chip(i, frm)[0]], br.at[i * 2 + frm])
        recv(results.at[z * 2 + 1 - core], br.at[1 - core])

    high = combine.astype(BF16).astype(F32)
    both = jnp.concatenate([high, combine - high], axis=0)[:, : ne * CAP].astype(BF16)
    for e in range(0, ne, 8):
        wide[e * 16 : (e + 8) * 16, :] = results[e : e + 8].astype(F32).reshape(128, 128)
    for j in range(jw):
        got = wide[pl.ds(j, ne * CAP, stride=jw), :].astype(BF16)
        part = jnp.dot(both, got, preferred_element_type=F32)
        out_ref[:, j * 128 : (j + 1) * 128] = (part[:4] + part[4:]).astype(BF16)
    for copy in c.sent:
        copy.wait_send()


def solution(mesh):
    nz = mesh.shape["seq"] // 2

    def step(*args):
        tokens, routes, fixed, gate, _, down, gs, us, ds_ = args
        dw, f1 = gate.shape[1:]
        nc, ni = CHUNKS, nz // CHUNKS
        m = NX * ni * 2 * CAP
        share = m // NX
        ne = 2 * nz
        dma = pltpu.SemaphoreType.DMA
        scratch = [
            pltpu.VMEM(tokens.shape, BF16),
            pltpu.VMEM(routes.shape, jnp.int32),
            pltpu.VMEM(fixed.shape, jnp.int32),
            pltpu.VMEM((dw, 2 * f1), BF16),
            pltpu.VMEM((f1, dw), BF16),
            pltpu.VMEM(gs.shape, BF16),
            pltpu.VMEM(us.shape, BF16),
            pltpu.VMEM(ds_.shape, BF16),
            pltpu.VMEM((dw // QB, 2 * f1), F32),
            pltpu.VMEM((f1 // QB, dw), F32),
            pltpu.VMEM((ne, 16, 128), BF16),
            pltpu.VMEM((NX, nz, 2, 16, 128), BF16),
            pltpu.VMEM((max(m, ne * CAP) * 8, 128), F32),
            pltpu.VMEM((m, dw), BF16),
            pltpu.VMEM((nc, 2, NX, share, f1), BF16),
            pltpu.VMEM((nc, 3, 2, share, f1), BF16),
            pltpu.VMEM((nc, NX, share, f1), BF16),
            pltpu.VMEM((nc, 2, NX, share, dw // 2), BF16),
            pltpu.VMEM((nc, 3, 2, share, dw // 2), BF16),
            pltpu.VMEM((share * 8, 128), F32),
            pltpu.VMEM((nc, ni, 2, 16, 128), BF16),
            pltpu.VMEM((ne, 16, 128), BF16),
            dma((9,)),
            dma((2 * nz,)),
            dma((2 * nz,)),
            dma((nc, 3)),
            dma((nc, 3)),
            dma((nc, 6)),
            dma((nc, 6)),
            dma((nc, 3)),
            dma((nc, 3)),
            dma((nc, 6)),
            dma((nc, 6)),
            dma((2 * nz,)),
            dma((2 * nz,)),
        ]
        return pl.pallas_call(
            functools.partial(kernel, nz),
            out_shape=jax.ShapeDtypeStruct(tokens.shape, BF16),
            in_specs=[pl.BlockSpec(memory_space=pltpu.HBM)] * 9,
            out_specs=pl.BlockSpec(memory_space=pltpu.VMEM),
            scratch_shapes=scratch,
            compiler_params=pltpu.CompilerParams(
                collective_id=0, has_side_effects=True, vmem_limit_bytes=60 * 1024 * 1024
            ),
        )(*args)

    return jax.shard_map(
        step,
        mesh=mesh,
        in_specs=(
            P(("seq", "head"), "pool"),
            P(("seq", "head"), None),
            P(("seq", "head"), None),
            P("seq", "pool", "head"),
            P("seq", "pool", "head"),
            P("seq", "head", "pool"),
            P("seq", "pool", "head"),
            P("seq", "pool", "head"),
            P("seq", "head", "pool"),
        ),
        out_specs=P(("seq", "head"), "pool"),
        check_vma=False,
    )
```

```python
import functools

import jax
import jax.numpy as jnp
from jax import lax
from jax.experimental import pallas as pl
from jax.experimental.pallas import tpu as pltpu
from jax.sharding import PartitionSpec as P

QB = 128
CAP = 2
NX = 4
CHUNKS = 4
ORDER = [divmod(n, 10) for n in (0, 1, 2, 10, 3, 11, 12, 20, 13, 21, 22, 30, 23, 31, 32, 40, 33, 41, 42, 43)]
F32 = jnp.float32
BF16 = jnp.bfloat16


def offset(i):
    k = (i + 1) // 2
    return k if i % 2 == 0 else -k


def opposite(i, nz):
    if i == 0:
        return 0
    other = i + 1 if i % 2 else i - 1
    return other if other < nz else i


def send(src, dst, send_sem, recv_sem, device):
    pltpu.make_async_remote_copy(
        src_ref=src,
        dst_ref=dst,
        send_sem=send_sem,
        recv_sem=recv_sem,
        device_id=device,
        device_id_type=pl.DeviceIdType.MESH,
    ).start()


def kernel(
    nz,
    tokens_hbm,
    routes_hbm,
    fixed_hbm,
    gate_hbm,
    up_hbm,
    down_hbm,
    gs_hbm,
    us_hbm,
    ds_hbm,
    out_ref,
    tokens,
    routes,
    fixed,
    w1,
    w2,
    gs,
    us,
    ds_,
    grown1,
    grown2,
    slots,
    gathered,
    wide,
    x_ref,
    partial,
    arrive_y,
    hidden,
    outs,
    arrive_x,
    back_wide,
    back,
    results,
    load_sem,
    zs,
    zr,
    gx_s,
    gx_r,
    ry_s,
    ry_r,
    gy_s,
    gy_r,
    rx_s,
    rx_r,
    bs,
    br,
):
    s = lax.axis_index("seq")
    h = lax.axis_index("head")
    p = lax.axis_index("pool")
    z = lax.div(s, 2)
    core = lax.rem(s, 2)
    nc = CHUNKS
    ni = nz // nc
    ne = 2 * nz
    m = NX * ni * 2 * CAP
    share = m // NX
    f1 = w1.shape[1] // 2
    dw = w2.shape[1]
    jw = dw // 128

    def near(base, step):
        return lax.rem(base + (step + NX), NX)

    xr, xl, xo = near(h, 1), near(h, -1), near(h, 2)
    yr, yl, yo = near(p, 1), near(p, -1), near(p, 2)
    devs_x = [(s, a, p) for a in (xo, xr, xl)]
    devs_y = [(s, h, a) for a in (yo, yr, yl)]

    def chip(i, to_core):
        return (lax.rem(z + (offset(i) + nz), nz) * 2 + to_core, h, p)

    barrier = pltpu.get_barrier_semaphore()
    for i in range(nz - 1, 0, -1):
        for c in (0, 1):
            pl.semaphore_signal(barrier, inc=1, device_id=chip(i, c), device_id_type=pl.DeviceIdType.MESH)
    for dev in (chip(0, 1 - core), *devs_x, *devs_y):
        pl.semaphore_signal(barrier, inc=1, device_id=dev, device_id_type=pl.DeviceIdType.MESH)

    loads = [
        (tokens_hbm, tokens),
        (routes_hbm, routes),
        (fixed_hbm, fixed),
        (gs_hbm, gs),
        (us_hbm, us),
        (ds_hbm, ds_),
        (gate_hbm.at[0], w1.at[:, pl.ds(0, f1)]),
        (up_hbm.at[0], w1.at[:, pl.ds(f1, f1)]),
        (down_hbm.at[0], w2),
    ]
    loads = [pltpu.make_async_copy(a, b, load_sem.at[n]) for n, (a, b) in enumerate(loads)]
    for load in loads:
        load.start()
    for load in loads[:3]:
        load.wait()

    lane = lax.broadcasted_iota(jnp.int32, (4, 128), 1)
    ids = routes[...]
    gates = fixed[...].astype(F32)
    weights = gates / jnp.sum(gates, axis=1, keepdims=True)
    names = jnp.zeros((4, 128), F32)
    weight = jnp.zeros((4, 128), F32)
    for k in range(ids.shape[1]):
        hit = ids[:, k : k + 1] == lane // CAP
        names = names + jnp.where(hit, 1.0, 0.0)
        weight = weight + jnp.where(hit, weights[:, k : k + 1], 0.0)
    before = [jnp.zeros((1, 128), F32)]
    for r in range(3):
        before.append(before[-1] + names[r : r + 1])
    before = jnp.concatenate(before, axis=0)
    selected = (names > 0.5) & (before == (lane % CAP).astype(F32))
    pick = jnp.where(selected, 1.0, 0.0)
    combine = jnp.where(selected, weight, 0.0)
    pick = jnp.concatenate([pick, jnp.zeros((4, 128), F32)], axis=0)
    pick = pick.T.astype(BF16)
    rows = tokens[...].astype(F32)
    rows = jnp.concatenate([rows, jnp.zeros_like(rows)], axis=0).astype(BF16)
    for j in range(jw):
        part = jnp.dot(pick, rows[:, j * 128 : (j + 1) * 128], preferred_element_type=F32)
        wide[pl.ds(j, ne * CAP, stride=jw), :] = part[: ne * CAP]
    for e in range(0, ne, 8):
        slots[e : e + 8] = wide[e * 16 : (e + 8) * 16, :].reshape(8, 16, 128).astype(BF16)

    with jax.named_scope("greet"):
        pl.semaphore_wait(barrier, 2 * (nz - 1) + 7)

    gathered[h, 0, core] = slots[s]
    send(slots.at[z * 2 + 1 - core], gathered.at[h, 0, core], zs.at[0], zr.at[0], chip(0, 1 - core))
    for i in range(1, nz):
        there = opposite(i, nz)
        for to in (0, 1):
            dev = chip(i, to)
            send(
                slots.at[dev[0]],
                gathered.at[h, there, core],
                zs.at[0],
                zr.at[there // ni],
                dev,
            )

    with jax.named_scope("loads"):
        for load in loads[3:]:
            load.wait()

    def grow(scale, count):
        v = scale[0].astype(F32)
        return jnp.concatenate(
            [jnp.broadcast_to(v[:, j : j + 1], (v.shape[0], 128)) for j in range(count)], axis=1
        )

    grown1[:, :f1] = grow(gs, f1 // QB)
    grown1[:, f1:] = grow(us, f1 // QB)
    grown2[...] = grow(ds_, dw // QB)

    def scale_w1(n, _):
        at = pl.ds(pl.multiple_of(n * 32, 32), 32)
        by = grown1[pl.ds(n // 4, 1), :]
        for half in (0, 1):
            cols = slice(half * f1, (half + 1) * f1)
            w1[at, cols] = (w1[at, cols].astype(F32) * by[:, cols]).astype(BF16)
        return 0

    def scale_w2(n, _):
        at = pl.ds(pl.multiple_of(n * 32, 32), 32)
        w2[at, :] = (w2[at, :].astype(F32) * grown2[pl.ds(n // 4, 1), :]).astype(BF16)
        return 0

    with jax.named_scope("scale"):
        lax.fori_loop(0, w1.shape[0] // 32, scale_w1, 0)
        lax.fori_loop(0, w2.shape[0] // 32, scale_w2, 0)

    def span(k):
        return pl.ds(k * ni, ni)

    def take(size, sem):
        pltpu.make_async_copy(size, size, sem).wait()

    def stage0(k):
        take(slots.at[pl.ds(0, 2 * ni - (k == 0))], zr.at[k])
        block = gathered.at[h, span(k)]
        for n, dev in enumerate(devs_x):
            send(block, block, gx_s.at[0], gx_r.at[k], dev)

    def stage1(k):
        per = ni * 2 * 16
        take(gathered.at[pl.ds(0, 3), span(k)], gx_r.at[k])
        for a in range(NX):
            wide[a * per : (a + 1) * per, :] = (
                gathered[a, k * ni : (k + 1) * ni].astype(F32).reshape(per, 128)
            )
        for j in range(jw):
            x_ref[:, j * 128 : (j + 1) * 128] = wide[pl.ds(j, m, stride=jw), :].astype(BF16)
        for half in (0, 1):
            part = jnp.dot(x_ref[...], w1[:, half * f1 : (half + 1) * f1], preferred_element_type=F32)
            partial[k, half] = part.reshape(NX, share, f1).astype(BF16)
            for n, (to, dev) in enumerate(zip((yo, yr, yl), devs_y)):
                send(
                    partial.at[k, half, to],
                    arrive_y.at[k, n, half],
                    ry_s.at[0],
                    ry_r.at[k],
                    dev,
                )

    def total(mine, arrived, k, half):
        return mine.astype(F32) + (
            arrived[k, 0, half].astype(F32) + arrived[k, 1, half].astype(F32) + arrived[k, 2, half].astype(F32)
        )

    def stage2(k):
        take(arrive_y.at[k], ry_r.at[k])
        g = total(partial[k, 0, p], arrive_y, k, 0)
        u = total(partial[k, 1, p], arrive_y, k, 1)
        hidden[k, p] = (g / (1.0 + jnp.exp(-g)) * u).astype(BF16)
        block = hidden.at[k, p]
        for n, dev in enumerate(devs_y):
            send(block, block, gy_s.at[0], gy_r.at[k], dev)

    def stage3(k):
        take(hidden.at[k, pl.ds(0, 3)], gy_r.at[k])
        for half in (0, 1):
            act = hidden[k].reshape(m, f1)
            part = jnp.dot(act, w2[:, half * dw // 2 : (half + 1) * dw // 2], preferred_element_type=F32)
            outs[k, half] = part.reshape(NX, share, dw // 2).astype(BF16)
            for n, (to, dev) in enumerate(zip((xo, xr, xl), devs_x)):
                send(
                    outs.at[k, half, to],
                    arrive_x.at[k, n, half],
                    rx_s.at[0],
                    rx_r.at[k],
                    dev,
                )

    def stage4(k):
        take(arrive_x.at[k], rx_r.at[k])
        for n in (0, 1):
            y = total(outs[k, n, h], arrive_x, k, n)
            for j in range(jw // 2):
                back_wide[pl.ds(n * (jw // 2) + j, share, stride=jw), :] = y[:, j * 128 : (j + 1) * 128]
        back[k] = back_wide[...].reshape(ni, 2, 16, 128).astype(BF16)
        for n in reversed(range(ni)):
            i = k * ni + n
            for to in (0, 1):
                if i == 0:
                    continue
                there = opposite(i, nz)
                send(
                    back.at[k, n, to],
                    results.at[s],
                    bs.at[0],
                    br.at[there // (nz - ni)],
                    chip(i, to),
                )
        if k == 0:
            send(back.at[0, 0, 1 - core], results.at[s], bs.at[0], br.at[0], chip(0, 1 - core))
            results[s] = back[0, 0, core]

    stages = [stage0, stage1, stage2, stage3, stage4]
    for n, k in ORDER:
        with jax.named_scope(f"s{n}c{k}"):
            stages[n](k)

    with jax.named_scope("drain"):
        take(slots.at[pl.ds(0, ne - 1)], zs.at[0])
        take(gathered.at[pl.ds(0, 3)], gx_s.at[0])
        take(arrive_y, ry_s.at[0])
        take(hidden.at[:, pl.ds(0, 3)], gy_s.at[0])
        take(arrive_x, rx_s.at[0])

    def widen(i):
        at = chip(i, 0)[0]
        rows_ = pl.ds(pl.multiple_of(at * 16, 32), 32)
        wide[rows_, :] = results[pl.ds(at, 2)].astype(F32).reshape(32, 128)

    far = 2 * ni
    with jax.named_scope("back"):
        take(results.at[pl.ds(0, ne - 1 - far)], br.at[0])
        for i in range(nz - ni):
            widen(i)
        take(slots.at[pl.ds(0, ne - 1)], bs.at[0])
        take(results.at[pl.ds(0, far)], br.at[1])
        for i in range(nz - ni, nz):
            widen(i)

    high = combine.astype(BF16).astype(F32)
    both = jnp.concatenate([high, combine - high], axis=0)[:, : ne * CAP].astype(BF16)
    for j in range(jw):
        x_ref[: ne * CAP, j * 128 : (j + 1) * 128] = wide[pl.ds(j, ne * CAP, stride=jw), :].astype(BF16)
    part = jnp.dot(both, x_ref[: ne * CAP], preferred_element_type=F32)
    out_ref[...] = (part[:4] + part[4:]).astype(BF16)


def solution(mesh):
    nz = mesh.shape["seq"] // 2

    def step(*args):
        tokens, routes, fixed, gate, _, down, gs, us, ds_ = args
        dw, f1 = gate.shape[1:]
        nc, ni = CHUNKS, nz // CHUNKS
        m = NX * ni * 2 * CAP
        share = m // NX
        ne = 2 * nz
        dma = pltpu.SemaphoreType.DMA
        scratch = [
            pltpu.VMEM(tokens.shape, BF16),
            pltpu.VMEM(routes.shape, jnp.int32),
            pltpu.VMEM(fixed.shape, jnp.int32),
            pltpu.VMEM((dw, 2 * f1), BF16),
            pltpu.VMEM((f1, dw), BF16),
            pltpu.VMEM(gs.shape, BF16),
            pltpu.VMEM(us.shape, BF16),
            pltpu.VMEM(ds_.shape, BF16),
            pltpu.VMEM((dw // QB, 2 * f1), F32),
            pltpu.VMEM((f1 // QB, dw), F32),
            pltpu.VMEM((ne, 16, 128), BF16),
            pltpu.VMEM((NX, nz, 2, 16, 128), BF16),
            pltpu.VMEM((max(m, ne * CAP) * 8, 128), F32),
            pltpu.VMEM((m, dw), BF16),
            pltpu.VMEM((nc, 2, NX, share, f1), BF16),
            pltpu.VMEM((nc, 3, 2, share, f1), BF16),
            pltpu.VMEM((nc, NX, share, f1), BF16),
            pltpu.VMEM((nc, 2, NX, share, dw // 2), BF16),
            pltpu.VMEM((nc, 3, 2, share, dw // 2), BF16),
            pltpu.VMEM((share * 8, 128), F32),
            pltpu.VMEM((nc, ni, 2, 16, 128), BF16),
            pltpu.VMEM((ne, 16, 128), BF16),
            dma((9,)),
            dma((1,)),
            dma((nc,)),
            dma((1,)),
            dma((nc,)),
            dma((1,)),
            dma((nc,)),
            dma((1,)),
            dma((nc,)),
            dma((1,)),
            dma((nc,)),
            dma((1,)),
            dma((2,)),
        ]
        return pl.pallas_call(
            functools.partial(kernel, nz),
            out_shape=jax.ShapeDtypeStruct(tokens.shape, BF16),
            in_specs=[pl.BlockSpec(memory_space=pltpu.HBM)] * 9,
            out_specs=pl.BlockSpec(memory_space=pltpu.VMEM),
            scratch_shapes=scratch,
            compiler_params=pltpu.CompilerParams(
                collective_id=0, has_side_effects=True, vmem_limit_bytes=60 * 1024 * 1024
            ),
        )(*args)

    return jax.shard_map(
        step,
        mesh=mesh,
        in_specs=(
            P(("seq", "head"), "pool"),
            P(("seq", "head"), None),
            P(("seq", "head"), None),
            P("seq", "pool", "head"),
            P("seq", "pool", "head"),
            P("seq", "head", "pool"),
            P("seq", "pool", "head"),
            P("seq", "pool", "head"),
            P("seq", "head", "pool"),
        ),
        out_specs=P(("seq", "head"), "pool"),
        check_vma=False,
    )
```

```python
import functools

import jax
import jax.numpy as jnp
from jax import lax
from jax.experimental import pallas as pl
from jax.experimental.pallas import tpu as pltpu
from jax.sharding import PartitionSpec as P

QB = 128
CAP = 2
NX = 4
CHUNKS = 4
ORDER = [divmod(n, 10) for n in (3, 2, 1, 0, 13, 12, 11, 23, 10, 22, 21, 33, 20, 32, 31, 43, 30, 42, 41, 40)]
F32 = jnp.float32
BF16 = jnp.bfloat16


def offset(i):
    k = (i + 1) // 2
    return k if i % 2 == 0 else -k


def opposite(i, nz):
    if i == 0:
        return 0
    other = i + 1 if i % 2 else i - 1
    return other if other < nz else i


def send(src, dst, send_sem, recv_sem, device):
    pltpu.make_async_remote_copy(
        src_ref=src,
        dst_ref=dst,
        send_sem=send_sem,
        recv_sem=recv_sem,
        device_id=device,
        device_id_type=pl.DeviceIdType.MESH,
    ).start()


def kernel(
    nz,
    tokens_hbm,
    routes_hbm,
    fixed_hbm,
    gate_hbm,
    up_hbm,
    down_hbm,
    gs_hbm,
    us_hbm,
    ds_hbm,
    out_ref,
    tokens,
    routes,
    fixed,
    w1,
    w2,
    gs,
    us,
    ds_,
    grown1,
    grown2,
    slots,
    gathered,
    wide,
    x_ref,
    partial,
    arrive_y,
    hidden,
    outs,
    arrive_x,
    back_wide,
    back,
    results,
    load_sem,
    zs,
    zr,
    gx_s,
    gx_r,
    ry_s,
    ry_r,
    gy_s,
    gy_r,
    rx_s,
    rx_r,
    bs,
    br,
):
    s = lax.axis_index("seq")
    h = lax.axis_index("head")
    p = lax.axis_index("pool")
    z = lax.div(s, 2)
    core = lax.rem(s, 2)
    nc = CHUNKS
    ni = nz // nc
    ne = 2 * nz
    m = NX * ni * 2 * CAP
    share = m // NX
    f1 = w1.shape[1] // 2
    dw = w2.shape[1]
    jw = dw // 128

    def near(base, step):
        return lax.rem(base + (step + NX), NX)

    xr, xl, xo = near(h, 1), near(h, -1), near(h, 2)
    yr, yl, yo = near(p, 1), near(p, -1), near(p, 2)
    devs_x = [(s, a, p) for a in (xo, xr, xl)]
    devs_y = [(s, h, a) for a in (yo, yr, yl)]

    def chip(i, to_core):
        return (lax.rem(z + (offset(i) + nz), nz) * 2 + to_core, h, p)

    barrier = pltpu.get_barrier_semaphore()
    for i in range(nz - 1, 0, -1):
        for c in (0, 1):
            pl.semaphore_signal(barrier, inc=1, device_id=chip(i, c), device_id_type=pl.DeviceIdType.MESH)
    for dev in (chip(0, 1 - core), *devs_x, *devs_y):
        pl.semaphore_signal(barrier, inc=1, device_id=dev, device_id_type=pl.DeviceIdType.MESH)

    loads = [
        (tokens_hbm, tokens),
        (routes_hbm, routes),
        (fixed_hbm, fixed),
        (gs_hbm, gs),
        (us_hbm, us),
        (ds_hbm, ds_),
        (gate_hbm.at[0], w1.at[:, pl.ds(0, f1)]),
        (up_hbm.at[0], w1.at[:, pl.ds(f1, f1)]),
        (down_hbm.at[0], w2),
    ]
    loads = [pltpu.make_async_copy(a, b, load_sem.at[n]) for n, (a, b) in enumerate(loads)]
    for load in loads:
        load.start()
    for load in loads[:3]:
        load.wait()

    lane = lax.broadcasted_iota(jnp.int32, (4, 128), 1)
    ids = routes[...]
    gates = fixed[...].astype(F32)
    weights = gates / jnp.sum(gates, axis=1, keepdims=True)
    names = jnp.zeros((4, 128), F32)
    weight = jnp.zeros((4, 128), F32)
    for k in range(ids.shape[1]):
        hit = ids[:, k : k + 1] == lane // CAP
        names = names + jnp.where(hit, 1.0, 0.0)
        weight = weight + jnp.where(hit, weights[:, k : k + 1], 0.0)
    before = [jnp.zeros((1, 128), F32)]
    for r in range(3):
        before.append(before[-1] + names[r : r + 1])
    before = jnp.concatenate(before, axis=0)
    selected = (names > 0.5) & (before == (lane % CAP).astype(F32))
    pick = jnp.where(selected, 1.0, 0.0)
    combine = jnp.where(selected, weight, 0.0)
    pick = jnp.concatenate([pick, jnp.zeros((4, 128), F32)], axis=0)
    pick = pick.T.astype(BF16)
    rows = tokens[...].astype(F32)
    rows = jnp.concatenate([rows, jnp.zeros_like(rows)], axis=0).astype(BF16)
    for j in range(jw):
        part = jnp.dot(pick, rows[:, j * 128 : (j + 1) * 128], preferred_element_type=F32)
        wide[pl.ds(j, ne * CAP, stride=jw), :] = part[: ne * CAP]
    for e in range(0, ne, 8):
        slots[e : e + 8] = wide[e * 16 : (e + 8) * 16, :].reshape(8, 16, 128).astype(BF16)

    with jax.named_scope("greet"):
        pl.semaphore_wait(barrier, 2 * (nz - 1) + 7)

    gathered[h, 0, core] = slots[s]
    send(slots.at[z * 2 + 1 - core], gathered.at[h, 0, core], zs.at[0], zr.at[0], chip(0, 1 - core))
    for i in range(nz - 1, 0, -1):
        there = opposite(i, nz)
        for to in (0, 1):
            dev = chip(i, to)
            send(
                slots.at[dev[0]],
                gathered.at[h, there, core],
                zs.at[0],
                zr.at[there // ni],
                dev,
            )

    with jax.named_scope("loads"):
        for load in loads[3:]:
            load.wait()

    def grow(scale, count):
        v = scale[0].astype(F32)
        return jnp.concatenate(
            [jnp.broadcast_to(v[:, j : j + 1], (v.shape[0], 128)) for j in range(count)], axis=1
        )

    grown1[:, :f1] = grow(gs, f1 // QB)
    grown1[:, f1:] = grow(us, f1 // QB)
    grown2[...] = grow(ds_, dw // QB)

    def scale_w1(n, _):
        at = pl.ds(pl.multiple_of(n * 32, 32), 32)
        by = grown1[pl.ds(n // 4, 1), :]
        for half in (0, 1):
            cols = slice(half * f1, (half + 1) * f1)
            w1[at, cols] = (w1[at, cols].astype(F32) * by[:, cols]).astype(BF16)
        return 0

    def scale_w2(n, _):
        at = pl.ds(pl.multiple_of(n * 32, 32), 32)
        w2[at, :] = (w2[at, :].astype(F32) * grown2[pl.ds(n // 4, 1), :]).astype(BF16)
        return 0

    with jax.named_scope("scale"):
        lax.fori_loop(0, w1.shape[0] // 32, scale_w1, 0)
        lax.fori_loop(0, w2.shape[0] // 32, scale_w2, 0)

    def span(k):
        return pl.ds(k * ni, ni)

    def take(size, sem):
        pltpu.make_async_copy(size, size, sem).wait()

    def stage0(k):
        take(slots.at[pl.ds(0, 2 * ni - (k == 0))], zr.at[k])
        block = gathered.at[h, span(k)]
        for n, dev in enumerate(devs_x):
            send(block, block, gx_s.at[0], gx_r.at[k], dev)

    def stage1(k):
        per = ni * 2 * 16
        take(gathered.at[pl.ds(0, 3), span(k)], gx_r.at[k])
        for a in range(NX):
            wide[a * per : (a + 1) * per, :] = (
                gathered[a, k * ni : (k + 1) * ni].astype(F32).reshape(per, 128)
            )
        for j in range(jw):
            x_ref[:, j * 128 : (j + 1) * 128] = wide[pl.ds(j, m, stride=jw), :].astype(BF16)
        for half in (0, 1):
            part = jnp.dot(x_ref[...], w1[:, half * f1 : (half + 1) * f1], preferred_element_type=F32)
            partial[k, half] = part.reshape(NX, share, f1).astype(BF16)
            for n, (to, dev) in enumerate(zip((yo, yr, yl), devs_y)):
                send(
                    partial.at[k, half, to],
                    arrive_y.at[k, n, half],
                    ry_s.at[0],
                    ry_r.at[k],
                    dev,
                )

    def total(mine, arrived, k, half):
        return mine.astype(F32) + (
            arrived[k, 0, half].astype(F32) + arrived[k, 1, half].astype(F32) + arrived[k, 2, half].astype(F32)
        )

    def stage2(k):
        take(arrive_y.at[k], ry_r.at[k])
        g = total(partial[k, 0, p], arrive_y, k, 0)
        u = total(partial[k, 1, p], arrive_y, k, 1)
        hidden[k, p] = (g / (1.0 + jnp.exp(-g)) * u).astype(BF16)
        block = hidden.at[k, p]
        for n, dev in enumerate(devs_y):
            send(block, block, gy_s.at[0], gy_r.at[k], dev)

    def stage3(k):
        take(hidden.at[k, pl.ds(0, 3)], gy_r.at[k])
        for half in (0, 1):
            act = hidden[k].reshape(m, f1)
            part = jnp.dot(act, w2[:, half * dw // 2 : (half + 1) * dw // 2], preferred_element_type=F32)
            outs[k, half] = part.reshape(NX, share, dw // 2).astype(BF16)
            for n, (to, dev) in enumerate(zip((xo, xr, xl), devs_x)):
                send(
                    outs.at[k, half, to],
                    arrive_x.at[k, n, half],
                    rx_s.at[0],
                    rx_r.at[k],
                    dev,
                )

    def stage4(k):
        take(arrive_x.at[k], rx_r.at[k])
        for n in (0, 1):
            y = total(outs[k, n, h], arrive_x, k, n)
            for j in range(jw // 2):
                back_wide[pl.ds(n * (jw // 2) + j, share, stride=jw), :] = y[:, j * 128 : (j + 1) * 128]
        back[k] = back_wide[...].reshape(ni, 2, 16, 128).astype(BF16)
        for n in reversed(range(ni)):
            i = k * ni + n
            for to in (0, 1):
                if i == 0:
                    continue
                there = opposite(i, nz)
                send(
                    back.at[k, n, to],
                    results.at[s],
                    bs.at[0],
                    br.at[there // (nz - ni)],
                    chip(i, to),
                )
        if k == 0:
            send(back.at[0, 0, 1 - core], results.at[s], bs.at[0], br.at[0], chip(0, 1 - core))
            results[s] = back[0, 0, core]

    stages = [stage0, stage1, stage2, stage3, stage4]
    for n, k in ORDER:
        with jax.named_scope(f"s{n}c{k}"):
            stages[n](k)

    with jax.named_scope("drain"):
        take(slots.at[pl.ds(0, ne - 1)], zs.at[0])
        take(gathered.at[pl.ds(0, 3)], gx_s.at[0])
        take(arrive_y, ry_s.at[0])
        take(hidden.at[:, pl.ds(0, 3)], gy_s.at[0])
        take(arrive_x, rx_s.at[0])

    def widen(i):
        at = chip(i, 0)[0]
        rows_ = pl.ds(pl.multiple_of(at * 16, 32), 32)
        wide[rows_, :] = results[pl.ds(at, 2)].astype(F32).reshape(32, 128)

    far = 2 * ni
    with jax.named_scope("back"):
        take(results.at[pl.ds(0, ne - 1 - far)], br.at[0])
        for i in range(nz - ni):
            widen(i)
        take(slots.at[pl.ds(0, ne - 1)], bs.at[0])
        take(results.at[pl.ds(0, far)], br.at[1])
        for i in range(nz - ni, nz):
            widen(i)

    high = combine.astype(BF16).astype(F32)
    both = jnp.concatenate([high, combine - high], axis=0)[:, : ne * CAP].astype(BF16)
    for j in range(jw):
        x_ref[: ne * CAP, j * 128 : (j + 1) * 128] = wide[pl.ds(j, ne * CAP, stride=jw), :].astype(BF16)
    part = jnp.dot(both, x_ref[: ne * CAP], preferred_element_type=F32)
    out_ref[...] = (part[:4] + part[4:]).astype(BF16)


def solution(mesh):
    nz = mesh.shape["seq"] // 2

    def step(*args):
        tokens, routes, fixed, gate, _, down, gs, us, ds_ = args
        dw, f1 = gate.shape[1:]
        nc, ni = CHUNKS, nz // CHUNKS
        m = NX * ni * 2 * CAP
        share = m // NX
        ne = 2 * nz
        dma = pltpu.SemaphoreType.DMA
        scratch = [
            pltpu.VMEM(tokens.shape, BF16),
            pltpu.VMEM(routes.shape, jnp.int32),
            pltpu.VMEM(fixed.shape, jnp.int32),
            pltpu.VMEM((dw, 2 * f1), BF16),
            pltpu.VMEM((f1, dw), BF16),
            pltpu.VMEM(gs.shape, BF16),
            pltpu.VMEM(us.shape, BF16),
            pltpu.VMEM(ds_.shape, BF16),
            pltpu.VMEM((dw // QB, 2 * f1), F32),
            pltpu.VMEM((f1 // QB, dw), F32),
            pltpu.VMEM((ne, 16, 128), BF16),
            pltpu.VMEM((NX, nz, 2, 16, 128), BF16),
            pltpu.VMEM((max(m, ne * CAP) * 8, 128), F32),
            pltpu.VMEM((m, dw), BF16),
            pltpu.VMEM((nc, 2, NX, share, f1), BF16),
            pltpu.VMEM((nc, 3, 2, share, f1), BF16),
            pltpu.VMEM((nc, NX, share, f1), BF16),
            pltpu.VMEM((nc, 2, NX, share, dw // 2), BF16),
            pltpu.VMEM((nc, 3, 2, share, dw // 2), BF16),
            pltpu.VMEM((share * 8, 128), F32),
            pltpu.VMEM((nc, ni, 2, 16, 128), BF16),
            pltpu.VMEM((ne, 16, 128), BF16),
            dma((9,)),
            dma((1,)),
            dma((nc,)),
            dma((1,)),
            dma((nc,)),
            dma((1,)),
            dma((nc,)),
            dma((1,)),
            dma((nc,)),
            dma((1,)),
            dma((nc,)),
            dma((1,)),
            dma((2,)),
        ]
        return pl.pallas_call(
            functools.partial(kernel, nz),
            out_shape=jax.ShapeDtypeStruct(tokens.shape, BF16),
            in_specs=[pl.BlockSpec(memory_space=pltpu.HBM)] * 9,
            out_specs=pl.BlockSpec(memory_space=pltpu.VMEM),
            scratch_shapes=scratch,
            compiler_params=pltpu.CompilerParams(
                collective_id=0, has_side_effects=True, vmem_limit_bytes=60 * 1024 * 1024
            ),
        )(*args)

    return jax.shard_map(
        step,
        mesh=mesh,
        in_specs=(
            P(("seq", "head"), "pool"),
            P(("seq", "head"), None),
            P(("seq", "head"), None),
            P("seq", "pool", "head"),
            P("seq", "pool", "head"),
            P("seq", "head", "pool"),
            P("seq", "pool", "head"),
            P("seq", "pool", "head"),
            P("seq", "head", "pool"),
        ),
        out_specs=P(("seq", "head"), "pool"),
        check_vma=False,
    )
```
